128 devices in a mesh: gx: 8 (over x, core), gy: 16 (over y, z).
Axes of the slice: x: 4, y: 4, z: 4, core: 2. Of those that a mesh axis runs over, the one named last changes fastest.
Arguments:
- state: float32 [32, 768, 2048], P('gx', None, 'gy'), may hold values from -6 to 6
- forcing: float32 [32, 768, 2048], P('gx', None, 'gy'), may hold values from -6 to 6
- vertical_mix: float32 [768, 768], replicated, may hold values from -0.21875 to 0.21875
- diffusion: float32 [768], replicated, may hold values from 0.1 to 1
- column_class: int32 [32, 2048], P('gx', 'gy'), may hold values from 0 to 2
- block_regime: int32 [16, 32, 1], P('gy', 'gx'), may hold values from 0 to 7; in each aligned block of 4 rows (0 to 3, 4 to 7, ..., all dimensions but the last counted through in order) no two rows name the same one
- correction_ops: float32 [8, 768, 768], P('gx'), may hold values from -0.21875 to 0.21875
Outputs:
- new_state: float32 [32, 768, 2048], P('gx', None, 'gy')
The draws below stay inside these ranges and needn't reach their ends.
Inputs may be any that keep to these rules, and one draw needn't show every extreme that they name: `block_regime`: among the blocks of one device (the same first index, 4 consecutive grid rows) no regime appears twice.
All inputs are finite; a program needn't handle non-finite values.
Results may differ from the reference program's by a relative error of at most 0.0002.
Values sent between devices are 32-bit elements; how exact they have to be, the bound alone decides.
No kernel may reach another device: no remote copies, remote signals or barrier semaphores. Data moves between devices by JAX's collectives and lax.ppermute only.
A program may use at most 128 MiB of HBM per device.

```python
import math
import jax
import jax.numpy as jnp
import numpy as np
from jax import lax

CX = 4
CY = 128
ITERS = 4
PROFILE = 768
REGIMES = 8
NX = 32
NY = 2048
N_GY = 16


def plant(drawn, stream_key, smallest, largest):
    longest = drawn.shape.index(max(drawn.shape))
    spots = []
    for shift in (0, 1):
        where = [jax.random.randint(jax.random.fold_in(stream_key, axis), (), 0, length) for axis, length in enumerate(drawn.shape)]
        where[longest] = (where[longest] + shift) % drawn.shape[longest]
        spots.append(tuple(where))
    return drawn.at[spots[0]].set(smallest).at[spots[1]].set(largest)


def block_scale(own_key, dims, split, least, top_value):
    def one(position, blocks):
        heights = jax.random.uniform(jax.random.fold_in(jax.random.fold_in(own_key, 6), position), (blocks,), jnp.float32, least / len(split), top_value / len(split))
        return jnp.repeat(jnp.exp(heights), dims[position] // blocks).reshape((-1,) + (1,) * (len(dims) - position - 1))

    loudness = one(*split[0])
    for cut in split[1:]:
        loudness = loudness * one(*cut)
    return loudness


def shared_out(key, own, number, rows, count, top, bound, skew):
    order = jax.random.permutation(key, count)
    packed, ordinary = load_shares(count, rows * top, bound, skew, True), load_shares(count, rows * top, bound, skew, False)
    places = jnp.arange(count)

    def named(tallies, rotation):
        used = int((tallies > 0).sum())
        fixed = max(1, used // 4)
        shifted = fixed + (places - fixed + rotation * (used - fixed)) % max(1, count - fixed)
        return jnp.zeros((count,), jnp.int32).at[order[jnp.where(places < fixed, places, shifted)]].set(jnp.asarray(tallies, jnp.int32))

    tallies = jnp.where(number % 4 == 0, named(packed, number // 4), named(ordinary, number - number // 4 - 1))
    mixed = jax.random.permutation(jax.random.fold_in(own, 3), count)
    source_of, receiver = mixed[0:count // 2 * 2:2], mixed[1:count // 2 * 2:2]
    slack = jnp.minimum(tallies[source_of] - 1, bound - tallies[receiver]) // 2
    slack = jnp.where((source_of == order[0]) | (receiver == order[0]) | (tallies[receiver] == 0), 0, jnp.maximum(slack, 0))
    shifted = jax.random.randint(jax.random.fold_in(own, 4), (count // 2,), 0, 1 << 20) % (slack + 1)
    tallies = tallies.at[source_of].add(-shifted).at[receiver].add(shifted)
    members = jnp.searchsorted(jnp.cumsum(tallies), jnp.arange(rows * top), side="right").astype(jnp.int32)
    table = members.reshape(top, rows).T
    table = table[jax.random.permutation(jax.random.fold_in(own, 1), rows)]
    rotation = jax.random.randint(jax.random.fold_in(own, 2), (rows, 1), 0, top)
    return jnp.take_along_axis(table, (jnp.arange(top)[None, :] + rotation) % top, axis=1)


def load_shares(amount, total, limit, lean, full):
    portions = [(1 << 20) // math.isqrt(rank ** lean) + 1 for rank in range(1, amount + 1)]
    largest = limit if full else min(limit, max(-(-total // amount), total * portions[0] // sum(portions)))
    least = 1 if total - largest >= amount - 1 else 0
    counts, surplus = [largest] + [least] * (amount - 1), total - largest - least * (amount - 1)
    while surplus > 0:
        movable = [i for i in range(1, amount) if counts[i] < largest] or [i for i in range(1, amount) if counts[i] < limit]
        whole, budget = sum([portions[i] for i in movable]), surplus
        for i in movable:
            addition = min(limit - counts[i], max(1, budget * portions[i] // whole), surplus)
            counts[i] = counts[i] + addition
            surplus = surplus - addition
    return np.array(counts)


def centred(key, shape, deviation, reach, split=(), dtype=jnp.bfloat16):
    gain = block_scale(key, shape, split, -0.22, 0.18) if split else 1.0
    array = jax.random.normal(key, shape, jnp.float32) * deviation * gain
    return jnp.minimum(jnp.maximum(array, -reach), reach).astype(dtype)


def setup_inputs(seed: int = 0) -> dict:
    streams_of = jax.random.split(jax.random.key(seed), 8)
    state = centred(streams_of[0], (NX, PROFILE, NY), 1.0, 6.0, ((0, 8), (2, 16)), jnp.float32)
    forcing = centred(streams_of[1], (NX, PROFILE, NY), 1.0, 6.0, ((0, 8), (2, 16)), jnp.float32)
    vertical_mix = centred(streams_of[2], (PROFILE, PROFILE), PROFILE ** -0.5, 0.21875, (), jnp.float32)
    diffusion = jnp.clip(jnp.exp(jax.random.uniform(streams_of[3], (PROFILE,), jnp.float32, math.log(0.1), math.log(1.0))), 0.1, 1.0)
    column_class = plant(jax.random.randint(streams_of[4], (NX, NY), 0, 3), jax.random.fold_in(streams_of[4], 1), 0, 2).astype(jnp.int32)
    block_regime_keys = jax.random.split(jax.random.fold_in(streams_of[5], 1), N_GY * NX // CX)
    block_regime_turns = jax.random.permutation(jax.random.fold_in(streams_of[5], 3), N_GY * NX // CX)
    block_regime = jax.vmap(lambda own, number: shared_out(jax.random.fold_in(streams_of[5], 2), own, number, CX, REGIMES, 1, 1, 2))(block_regime_keys, block_regime_turns).reshape((N_GY, NX, 1))
    correction_ops = centred(streams_of[6], (REGIMES, PROFILE, PROFILE), PROFILE ** -0.5, 0.21875, ((0, 8),), jnp.float32)
    return dict(state=state, forcing=forcing, vertical_mix=vertical_mix, diffusion=diffusion, column_class=column_class, block_regime=block_regime, correction_ops=correction_ops)


def spread(field, vertical_mix, diffusion):
    padded = jnp.pad(field, ((1, 1), (0, 0), (1, 1)))
    centre = padded[1:-1, :, 1:-1]
    lap = 4.0 * centre - padded[2:, :, 1:-1] - padded[:-2, :, 1:-1] - padded[1:-1, :, 2:] - padded[1:-1, :, :-2]
    mixed = jnp.einsum('pq,xqy->xpy', vertical_mix, field, precision=lax.Precision.HIGHEST)
    return 2.0 * field + mixed + diffusion[None, :, None] * lap

def correct(field, block_regime, correction_ops, weights):

    def one_row(items):
        row, regimes, row_weight = items
        blocks = row.reshape(PROFILE, N_GY, CY).transpose(1, 0, 2)
        chosen = correction_ops[regimes]
        result = jnp.einsum('bpq,bqc->bpc', chosen, blocks, precision=lax.Precision.HIGHEST)
        return result.transpose(1, 0, 2).reshape(PROFILE, NY) * row_weight[None, :]
    return lax.map(one_row, (field, block_regime[:, :, 0].T, weights))

def chol_solve(factor, target):
    count = target.shape[0]
    forward = []
    for index in range(count):
        value = target[index]
        for other in range(index):
            value = value - factor[index, other] * forward[other]
        forward.append(value / factor[index, index])
    backward = [None] * count
    for index in range(count - 1, -1, -1):
        value = forward[index]
        for other in range(index + 1, count):
            value = value - factor[other, index] * backward[other]
        backward[index] = value / factor[index, index]
    return jnp.stack(backward)

def reference(state, forcing, vertical_mix, diffusion, column_class, block_regime, correction_ops):
    weights = column_class.astype(jnp.float32) * 0.5
    shade = jnp.tanh(state)
    slope = 1.0 - shade * shade
    residual = forcing - (spread(state, vertical_mix, diffusion) + correct(shade, block_regime, correction_ops, weights))
    beta = jnp.sqrt(jnp.sum(residual * residual) + 1e-12)
    basis = [residual / beta]
    columns = []
    for step in range(ITERS):
        current = basis[-1]
        image = spread(current, vertical_mix, diffusion) + correct(slope * current, block_regime, correction_ops, weights)
        coefs = jnp.stack([jnp.sum(vector * image) for vector in basis])
        for index in range(len(basis)):
            image = image - coefs[index] * basis[index]
        length = jnp.sqrt(jnp.sum(image * image) + 1e-12)
        column = jnp.concatenate([coefs, length[None], jnp.zeros((ITERS - step - 1,), jnp.float32)])
        columns.append(column)
        if step + 1 < ITERS:
            basis.append(image / length)
    hess = jnp.stack(columns, axis=1)
    gram = jnp.dot(hess.T, hess, precision=lax.Precision.HIGHEST)
    target = beta * hess[0]
    factor = jnp.linalg.cholesky(gram)
    coeffs = chol_solve(factor, target)
    new_state = state
    for index in range(ITERS):
        new_state = new_state + coeffs[index] * basis[index]
    return new_state
```

```python
import functools

import jax
import jax.numpy as jnp
from jax import lax
from jax.experimental import pallas as pl
from jax.experimental.pallas import tpu as pltpu
from jax.sharding import PartitionSpec as P

ITERS = 4
ROWS = 4
N = 768
C = 128
AMP_MAX = 1e4
ALL = ("gx", "gy")
F32 = jnp.float32
BF16 = jnp.bfloat16
VM = pl.BlockSpec(memory_space=pltpu.VMEM)
SM = pl.BlockSpec(memory_space=pltpu.SMEM)
HB = pl.BlockSpec(memory_space=pltpu.HBM)
FIELD = (ROWS, N, C)


def params(mib):
    return pltpu.CompilerParams(vmem_limit_bytes=mib << 20)


def cost(flops, moved):
    return pl.CostEstimate(flops=flops, bytes_accessed=moved, transcendentals=0)


def in_vmem(*arrays):
    return [pltpu.with_memory_space_constraint(a, pltpu.VMEM) for a in arrays]


def halves(value):
    high = value.astype(BF16)
    return high, (value - high.astype(F32)).astype(BF16)


def dot(left, right):
    return jnp.dot(left, right, preferred_element_type=F32)


def lanes(shape):
    return lax.broadcasted_iota(jnp.int32, shape, len(shape) - 1)


def folded(value):
    return value[:, :C] + value[:, C:]


def local_lap(field, row):
    here = field(row)
    lane = lanes((N, C))
    total = 4.0 * here
    if row > 0:
        total = total - field(row - 1)
    if row + 1 < ROWS:
        total = total - field(row + 1)
    left = jnp.where(lane == 0, 0.0, pltpu.roll(here, 1, 1))
    right = jnp.where(lane == C - 1, 0.0, pltpu.roll(here, C - 1, 1))
    return total - left - right


def halo_terms(flags, up, down, left, right):
    pick = lax.broadcasted_iota(jnp.int32, (8, N), 0) % 2 == 0
    has_left = jnp.where(flags[2] > 0, left[...], 0.0)
    has_right = jnp.where(flags[3] > 0, right[...], 0.0)
    sides = jnp.concatenate([jnp.where(pick, has_left, has_right), jnp.zeros((C - 8, N), F32)], axis=0).T
    lane = lanes((N, C))
    out = []
    for row in range(ROWS):
        low = pltpu.roll(sides, (C - 2 * row) % C, 1)
        high = pltpu.roll(sides, (C - 1 - (2 * row + 1)) % C, 1)
        term = jnp.where(lane == 0, low, jnp.where(lane == C - 1, high, 0.0))
        if row == 0:
            term = term + jnp.where(flags[0] > 0, up[...], 0.0)
        if row == ROWS - 1:
            term = term + jnp.where(flags[1] > 0, down[...], 0.0)
        out.append(term)
    return out


def edge_rows(field):
    lane = lanes((N, C))
    tile = jnp.zeros((N, C), F32)
    for row in range(ROWS):
        moved = pltpu.roll(field(row), 2 * row + 1, 1)
        tile = jnp.where((lane == 2 * row) | (lane == 2 * row + 1), moved, tile)
    return tile.T[:8]


def mix_products(high, low, fields):
    splits = [halves(f) for f in fields]
    outs = [folded(dot(high, jnp.concatenate(s, axis=1))) for s in splits]
    for pair in range(0, ROWS, 2):
        both = dot(low, jnp.concatenate([splits[pair][0], splits[pair + 1][0]], axis=1))
        outs[pair] = outs[pair] + both[:, :C]
        outs[pair + 1] = outs[pair + 1] + both[:, C:]
    return outs


def op_product(high, low, field):
    fh, fl = halves(field)
    return folded(dot(high, jnp.concatenate([fh, fl], axis=1))) + dot(low, fh)


def edges_kernel(state, edges, first, last):
    edges[...] = edge_rows(lambda row: state[row])
    first[...] = state[0]
    last[...] = state[ROWS - 1]


def prep_kernel(flags, state, forcing, mix, coeff, weights, up, down, left, right, part, shade_out, slope_out, mix_hi, mix_lo):
    high, low = halves(mix[...])
    mix_hi[...] = high
    mix_lo[...] = low
    halo = halo_terms(flags, up, down, left, right)
    products = mix_products(high, low, [state[row] for row in range(ROWS)])
    d = coeff[...]
    for row in range(ROWS):
        here = state[row]
        lap = local_lap(lambda r: state[r], row) - halo[row]
        part[row] = forcing[row] - (2.0 * here + products[row] + d * lap)
        shade = jnp.tanh(here)
        shade_out[row] = shade * weights[row]
        slope_out[row] = (1.0 - shade * shade) * weights[row]


def residual_kernel(regimes, ops, part, shade, resid, edges, first, last, op_hi, op_lo, held, sems):
    copies = [pltpu.make_async_copy(ops.at[regimes[row]], held.at[row], sems.at[row]) for row in range(ROWS)]
    for copy in copies:
        copy.start()
    for row in range(ROWS):
        copies[row].wait()
        high, low = halves(held[row])
        op_hi[row] = high
        op_lo[row] = low
        resid[row] = part[row] - op_product(high, low, shade[row])
    edges[...] = edge_rows(lambda row: resid[row])
    first[...] = resid[0]
    last[...] = resid[ROWS - 1]


def sum_all(values):
    return jnp.sum(jnp.sum(values, axis=0, keepdims=True), axis=1, keepdims=True)


def gram_row(fields, newest, base):
    lane = lanes((8, C))
    out = jnp.zeros((8, C), F32)
    for index, other in enumerate(fields):
        total = jnp.zeros((8, C), F32)
        for row in range(ROWS):
            total = total + jnp.sum((newest[row] * other[row]).reshape(N // 8, 8, C), axis=0)
        out = jnp.where(lane == base + index, sum_all(total), out)
    return out


def apply_kernel(count, shift, *refs):
    earlier, (slope, mix_hi, mix_lo, op_hi, op_lo, coeff, image, gram) = refs[:count], refs[count:]
    newest = earlier[-1]
    products = mix_products(mix_hi[...], mix_lo[...], [newest[row] for row in range(ROWS)])
    d = coeff[...]
    centre = 2.0 - shift[0]
    for row in range(ROWS):
        here = newest[row]
        image[row] = (
            products[row]
            + op_product(op_hi[row], op_lo[row], slope[row] * here)
            + (centre * here + d * local_lap(lambda r: newest[r], row))
        )
    gram[...] = gram_row(earlier, newest, count * (count - 1) // 2)


def finish_kernel(flags, image, coeff, up, down, left, right, vector, edges, first, last):
    halo = halo_terms(flags, up, down, left, right)
    d = coeff[...]
    for row in range(ROWS):
        vector[row] = image[row] - d * halo[row]
    edges[...] = edge_rows(lambda row: vector[row])
    first[...] = vector[0]
    last[...] = vector[ROWS - 1]


def last_kernel(flags, image, coeff, up, down, left, right, *refs):
    earlier, grams, (out, vector) = refs[:4], refs[4:8], refs[8:]
    halo = halo_terms(flags, up, down, left, right)
    d = coeff[...]
    for row in range(ROWS):
        vector[row] = image[row] - d * halo[row]
    total = gram_row(list(earlier) + [vector], vector, 10)
    for gram in grams:
        total = total + gram[...]
    out[...] = jnp.broadcast_to(total[:1], (128, C))


def combination(sums, shift):
    lane = lanes((1, C))
    width = ITERS + 1

    def entry(index):
        return jnp.sum(jnp.where(lane == index, sums, 0.0), axis=1, keepdims=True)

    gram = [[None] * width for _ in range(width)]
    for i in range(width):
        for j in range(i + 1):
            gram[i][j] = gram[j][i] = entry(i * (i + 1) // 2 + j)

    def times(vec):
        return [sum(gram[a][b] * vec[b] for b in range(width) if vec[b] is not None) for a in range(width)]

    def inner(vec, image):
        return sum(v * m for v, m in zip(vec, image) if v is not None)

    def less(vec, scale, other):
        return [v if o is None else (-scale * o if v is None else v - scale * o) for v, o in zip(vec, other)]

    beta = jnp.sqrt(gram[0][0] + 1e-12)
    basis = [[1.0 / beta] + [None] * ITERS]
    hess = {}
    worst = jnp.zeros((1, 1), F32)
    for step in range(ITERS):
        now = basis[-1]
        work = [None] * width
        for a in range(step + 2):
            moved = now[a - 1] if a > 0 else None
            kept = None if now[a] is None else shift * now[a]
            work[a] = moved if kept is None else (kept if moved is None else moved + kept)
        image = times(work)
        coefs = [inner(vec, image) for vec in basis]
        for index, coef in enumerate(coefs):
            hess[index, step] = coef
            work = less(work, coef, basis[index])
        square = inner(work, times(work))
        bound = sum(
            jnp.abs(work[a] * gram[a][b] * work[b]) for a in range(step + 2) for b in range(step + 2)
        )
        worst = jnp.where(bound <= AMP_MAX * square, worst, 1.0)
        length = jnp.sqrt(square + 1e-12)
        hess[step + 1, step] = length
        basis.append([None if v is None else v / length for v in work])

    normal = [[None] * ITERS for _ in range(ITERS)]
    for i in range(ITERS):
        for j in range(i + 1):
            normal[i][j] = sum(hess[k, i] * hess[k, j] for k in range(width) if (k, i) in hess and (k, j) in hess)
    factor = [[None] * ITERS for _ in range(ITERS)]
    for j in range(ITERS):
        value = normal[j][j]
        for k in range(j):
            value = value - factor[j][k] * factor[j][k]
        factor[j][j] = jnp.sqrt(value)
        for i in range(j + 1, ITERS):
            value = normal[i][j]
            for k in range(j):
                value = value - factor[i][k] * factor[j][k]
            factor[i][j] = value / factor[j][j]
    forward = []
    for i in range(ITERS):
        value = beta * hess[0, i]
        for k in range(i):
            value = value - factor[i][k] * forward[k]
        forward.append(value / factor[i][i])
    solved = [None] * ITERS
    for i in range(ITERS - 1, -1, -1):
        value = forward[i]
        for k in range(i + 1, ITERS):
            value = value - factor[k][i] * solved[k]
        solved[i] = value / factor[i][i]
    weights = []
    for a in range(ITERS):
        weights.append(sum(solved[i] * basis[i][a] for i in range(ITERS) if basis[i][a] is not None))
    total = sum(weights)
    worst = jnp.where(total - total == 0.0, worst, 1.0)
    return weights, worst


def update_kernel(shift, table, state, p0, p1, p2, p3, new_state, poor):
    sums = jnp.sum(table[...], axis=0, keepdims=True)
    weights, worst = combination(sums, shift[0])
    poor[...] = jnp.broadcast_to(worst, (1, C))
    for row in range(ROWS):
        new_state[row] = state[row] + (
            weights[0] * p0[row] + weights[1] * p1[row] + weights[2] * p2[row] + weights[3] * p3[row]
        )


def ring(size, step):
    return [(i, (i + step) % size) for i in range(size)]


def exchange(edges, first, last):
    gx, gy = lax.axis_size("gx"), lax.axis_size("gy")
    left = lax.ppermute(edges, "gy", ring(gy, 1))
    right = lax.ppermute(edges, "gy", ring(gy, -1))
    up = lax.ppermute(last, "gx", ring(gx, 1))
    down = lax.ppermute(first, "gx", ring(gx, -1))
    return up, down, left, right


def total_sum(value):
    return lax.psum(value, ALL)


def careful(state, forcing, mix, diffusion, weights, chosen, flags):
    highest = lax.Precision.HIGHEST
    d = diffusion[None, :, None]
    gx, gy = lax.axis_size("gx"), lax.axis_size("gy")
    keep = flags.astype(F32)

    def spread(field):
        up = lax.ppermute(field[-1:], "gx", ring(gx, 1)) * keep[0]
        down = lax.ppermute(field[:1], "gx", ring(gx, -1)) * keep[1]
        left = lax.ppermute(field[:, :, -1], "gy", ring(gy, 1)) * keep[2]
        right = lax.ppermute(field[:, :, 0], "gy", ring(gy, -1)) * keep[3]
        tall = jnp.concatenate([up, field, down], axis=0)
        wide = jnp.concatenate([left[:, :, None], field, right[:, :, None]], axis=2)
        lap = 4.0 * field - tall[2:] - tall[:-2] - wide[:, :, 2:] - wide[:, :, :-2]
        mixed = jnp.einsum("pq,xqy->xpy", mix, field, precision=highest)
        return 2.0 * field + mixed + d * lap

    def correct(field):
        return jnp.einsum("bpq,bqc->bpc", chosen, field, precision=highest) * weights

    shade = jnp.tanh(state)
    slope = 1.0 - shade * shade
    residual = forcing - (spread(state) + correct(shade))
    beta = jnp.sqrt(total_sum(jnp.sum(residual * residual)) + 1e-12)
    basis = jnp.zeros((ITERS + 1,) + FIELD, F32).at[0].set(residual / beta)

    def body(step, carry):
        basis, hess = carry
        current = lax.dynamic_index_in_dim(basis, step, 0, keepdims=False)
        image = spread(current) + correct(slope * current)
        coefs = total_sum(jnp.sum(basis * image[None], axis=(1, 2, 3)))
        image = image - jnp.sum(coefs[:, None, None, None] * basis, axis=0)
        length = jnp.sqrt(total_sum(jnp.sum(image * image)) + 1e-12)
        basis = lax.dynamic_update_index_in_dim(basis, image / length, step + 1, 0)
        column = jnp.where(jnp.arange(ITERS + 1) == step + 1, length, coefs)
        hess = jnp.where(jnp.arange(ITERS)[None, :] == step, column[:, None], hess)
        return basis, hess

    basis, hess = lax.fori_loop(0, ITERS, body, (basis, jnp.zeros((ITERS + 1, ITERS), F32)))
    gram = jnp.dot(hess.T, hess, precision=highest)
    target = beta * hess[0]
    factor = jnp.linalg.cholesky(gram)
    forward = []
    for i in range(ITERS):
        value = target[i]
        for k in range(i):
            value = value - factor[i, k] * forward[k]
        forward.append(value / factor[i, i])
    solved = [None] * ITERS
    for i in range(ITERS - 1, -1, -1):
        value = forward[i]
        for k in range(i + 1, ITERS):
            value = value - factor[k, i] * solved[k]
        solved[i] = value / factor[i, i]
    new_state = state
    for i in range(ITERS):
        new_state = new_state + solved[i] * basis[i]
    return new_state


def call(kernel, outs, ins, arrays, mib, flops, scratch=()):
    return pl.pallas_call(
        kernel,
        out_shape=outs,
        in_specs=ins,
        out_specs=[VM] * len(outs),
        scratch_shapes=list(scratch),
        compiler_params=params(mib),
        cost_estimate=cost(flops, 1 << 22),
    )(*arrays)


def local(state, forcing, vertical_mix, diffusion, column_class, block_regime, correction_ops):
    gx, gy = lax.axis_index("gx"), lax.axis_index("gy")
    last_x, last_y = lax.axis_size("gx") - 1, lax.axis_size("gy") - 1
    flags = jnp.stack([gx > 0, gx < last_x, gy > 0, gy < last_y]).astype(jnp.int32)
    regimes = block_regime[0, :, 0]
    weights = (column_class.astype(F32) * 0.5)[:, None, :]
    coeff = diffusion[:, None]
    shift = (2.0 + 4.0 * jnp.mean(diffusion) + jnp.trace(vertical_mix) / N)[None]

    field = pltpu.VMEM(FIELD, F32)
    plane = pltpu.VMEM((N, C), F32)
    edge = pltpu.VMEM((8, N), F32)
    mm = 2 * N * N * ROWS * C

    every_op = lax.all_gather(correction_ops, "gx", axis=0, tiled=True)

    edges, first, last = call(edges_kernel, [edge, plane, plane], [VM], [state], 8, 1 << 20)
    up, down, left, right = exchange(edges, first, last)
    square = pltpu.VMEM((N, N), BF16)
    part, shade, slope, mix_hi, mix_lo = call(
        prep_kernel,
        [field, field, field, square, square],
        [SM] + [VM] * 9,
        [flags, state, forcing, vertical_mix, coeff, weights, up, down, left, right],
        28,
        3 * mm,
    )
    stack = pltpu.VMEM((ROWS, N, N), BF16)
    vector, edges, first, last, op_hi, op_lo = call(
        residual_kernel,
        [field, edge, plane, plane, stack, stack],
        [SM, HB, VM, VM],
        [regimes, every_op] + in_vmem(part, shade),
        32,
        3 * mm,
        [pltpu.VMEM((ROWS, N, N), F32), pltpu.SemaphoreType.DMA((ROWS,))],
    )
    vectors, grams = [vector], []
    for step in range(ITERS):
        up, down, left, right = exchange(edges, first, last)
        count = step + 1
        image, gram = call(
            functools.partial(apply_kernel, count),
            [field, pltpu.VMEM((8, C), F32)],
            [SM] + [VM] * (count + 6),
            [shift] + in_vmem(*vectors, slope, mix_hi, mix_lo, op_hi, op_lo) + [coeff],
            30,
            6 * mm,
        )
        grams.append(gram)
        if step + 1 < ITERS:
            vector, edges, first, last = call(
                finish_kernel,
                [field, edge, plane, plane],
                [SM] + [VM] * 6,
                [flags] + in_vmem(image) + [coeff, up, down, left, right],
                16,
                1 << 20,
            )
            vectors.append(vector)
    sums = call(
        last_kernel,
        [jax.ShapeDtypeStruct((128, C), F32)],
        [SM] + [VM] * 14,
        [flags] + in_vmem(image) + [coeff, up, down, left, right] + in_vmem(*vectors, *grams),
        24,
        1 << 20,
        [pltpu.VMEM(FIELD, F32)],
    )[0]
    table = lax.all_to_all(sums, ALL, 0, 0, tiled=True)
    new_state, poor = call(
        update_kernel,
        [jax.ShapeDtypeStruct(FIELD, F32), jax.ShapeDtypeStruct((1, C), F32)],
        [SM] + [VM] * 6,
        [shift, table, state] + in_vmem(*vectors),
        24,
        1 << 20,
    )

    def again(_):
        return careful(state, forcing, vertical_mix, diffusion, weights, every_op[regimes], flags)

    return lax.cond(poor[0, 0] > 0.0, again, lambda kept: kept, new_state)


def solution(mesh):
    in_specs = (
        P("gx", None, "gy"),
        P("gx", None, "gy"),
        P(),
        P(),
        P("gx", "gy"),
        P("gy", "gx", None),
        P("gx", None, None),
    )
    return jax.shard_map(local, mesh=mesh, in_specs=in_specs, out_specs=P("gx", None, "gy"), check_vma=False)
```

```python
import functools

import jax
import jax.numpy as jnp
from jax import lax
from jax.experimental import pallas as pl
from jax.experimental.pallas import tpu as pltpu
from jax.sharding import Mesh
from jax.sharding import PartitionSpec as P

ITERS = 4
ROWS = 4
N = 768
C = 128
AMP_MAX = 1e4
ALL = ("x", "c", "y", "z")
GX = ("x", "c")
GY = ("y", "z")
HALF = N // 2
PIECE = N // 8
F32 = jnp.float32
BF16 = jnp.bfloat16
VM = pl.BlockSpec(memory_space=pltpu.VMEM)
SM = pl.BlockSpec(memory_space=pltpu.SMEM)
HB = pl.BlockSpec(memory_space=pltpu.HBM)
FIELD = (ROWS, N, C)


def params(mib):
    return pltpu.CompilerParams(vmem_limit_bytes=mib << 20)


def cost(flops, moved):
    return pl.CostEstimate(flops=flops, bytes_accessed=moved, transcendentals=0)


def in_vmem(*arrays):
    return [pltpu.with_memory_space_constraint(a, pltpu.VMEM) for a in arrays]


def in_hbm(*arrays):
    return [pltpu.with_memory_space_constraint(a, pltpu.HBM) for a in arrays]


def halves(value):
    high = value.astype(BF16)
    return high, (value - high.astype(F32)).astype(BF16)


def dot(left, right):
    return jnp.dot(left, right, preferred_element_type=F32)


def lanes(shape):
    return lax.broadcasted_iota(jnp.int32, shape, len(shape) - 1)


def folded(value):
    return value[:, :C] + value[:, C:]


def local_lap(field, row):
    here = field(row)
    lane = lanes((N, C))
    total = 4.0 * here
    if row > 0:
        total = total - field(row - 1)
    if row + 1 < ROWS:
        total = total - field(row + 1)
    left = jnp.where(lane == 0, 0.0, pltpu.roll(here, 1, 1))
    right = jnp.where(lane == C - 1, 0.0, pltpu.roll(here, C - 1, 1))
    return total - left - right


def halo_terms(flags, up, down, left, right):
    pick = lax.broadcasted_iota(jnp.int32, (8, N), 0) % 2 == 0
    has_left = jnp.where(flags[2] > 0, left[...], 0.0)
    has_right = jnp.where(flags[3] > 0, right[...], 0.0)
    sides = jnp.concatenate([jnp.where(pick, has_left, has_right), jnp.zeros((C - 8, N), F32)], axis=0).T
    lane = lanes((N, C))
    out = []
    for row in range(ROWS):
        low = pltpu.roll(sides, (C - 2 * row) % C, 1)
        high = pltpu.roll(sides, (C - 1 - (2 * row + 1)) % C, 1)
        term = jnp.where(lane == 0, low, jnp.where(lane == C - 1, high, 0.0))
        if row == 0:
            term = term + jnp.where(flags[0] > 0, up[...], 0.0)
        if row == ROWS - 1:
            term = term + jnp.where(flags[1] > 0, down[...], 0.0)
        out.append(term)
    return out


def edge_rows(field):
    lane = lanes((N, C))
    tile = jnp.zeros((N, C), F32)
    for row in range(ROWS):
        moved = pltpu.roll(field(row), 2 * row + 1, 1)
        tile = jnp.where((lane == 2 * row) | (lane == 2 * row + 1), moved, tile)
    return tile.T[:8]


def mix_products(high, low, fields):
    splits = [halves(f) for f in fields]
    outs = [folded(dot(high, jnp.concatenate(s, axis=1))) for s in splits]
    for pair in range(0, ROWS, 2):
        both = dot(low, jnp.concatenate([splits[pair][0], splits[pair + 1][0]], axis=1))
        outs[pair] = outs[pair] + both[:, :C]
        outs[pair + 1] = outs[pair + 1] + both[:, C:]
    return outs


def op_product(high, low, field):
    fh, fl = halves(field)
    return folded(dot(high, jnp.concatenate([fh, fl], axis=1))) + dot(low, fh)


def edges_kernel(state, edges, first, last):
    edges[...] = edge_rows(lambda row: state[row])
    first[...] = state[0]
    last[...] = state[ROWS - 1]


def prep_kernel(state, forcing, mix, coeff, weights, part, shade_out, slope_out, mix_hi, mix_lo, shift):
    whole = mix[...]
    high, low = halves(whole)
    mix_hi[...] = high
    mix_lo[...] = low
    diagonal = lax.broadcasted_iota(jnp.int32, (N, N), 0) == lanes((N, N))
    d = coeff[...]
    shift[...] = 2.0 + (4.0 * sum_all(d) + sum_all(jnp.where(diagonal, whole, 0.0))) / N
    products = mix_products(high, low, [state[row] for row in range(ROWS)])
    for row in range(ROWS):
        here = state[row]
        part[row] = forcing[row] - (2.0 * here + products[row] + d * local_lap(lambda r: state[r], row))
        shade = jnp.tanh(here)
        shade_out[row] = shade * weights[row]
        slope_out[row] = (1.0 - shade * shade) * weights[row]


def residual_kernel(place, regimes, flags, part, shade, coeff, up, down, left, right, *refs):
    near, far, rest = refs[:13], refs[13:26], refs[26:]
    resid, edges, first, last, op_hi, op_lo, held, sems = rest
    mine = pl.multiple_of(place[2] * HALF, HALF)
    other = pl.multiple_of(HALF - place[2] * HALF, HALF)

    def fetch(row, carry):
        regime = regimes[row]
        offset = lax.rem(lax.div(regime, 2) - place[0] + 4, 4)
        for same, pieces in ((True, near), (False, far)):
            own, low, high, top, bottom = pieces[:5]
            sides, ends = pieces[5:9], pieces[9:]
            here = (lax.rem(regime, 2) == place[1]) == same

            def take(source, start, rows):
                pltpu.make_async_copy(source, held.at[row, pl.ds(start, rows)], sems.at[row]).start()

            @pl.when(here & (offset == 0))
            def _():
                take(own, 0, N)

            for index, (shift, block) in enumerate(((3, low), (1, high))):

                @pl.when(here & (offset == shift))
                def _(index=index, block=block):
                    take(block, mine, HALF)
                    for q in range(4):
                        take(sides[q].at[index], other + q * PIECE, PIECE)

            @pl.when(here & (offset == 2))
            def _():
                take(top, mine, HALF // 2)
                take(bottom, mine + HALF // 2, HALF // 2)
                for q in range(4):
                    take(ends[q], other + q * PIECE, PIECE)

        return carry

    lax.fori_loop(0, ROWS, fetch, 0)
    halo = halo_terms(flags, up, down, left, right)
    d = coeff[...]
    for row in range(ROWS):
        resid[row] = part[row] + d * halo[row]
    for row in range(ROWS):
        pltpu.make_async_copy(near[0], held.at[row], sems.at[row]).wait()
        high, low = halves(held[row])
        op_hi[row] = high
        op_lo[row] = low
        resid[row] = resid[row] - op_product(high, low, shade[row])
    edges[...] = edge_rows(lambda row: resid[row])
    first[...] = resid[0]
    last[...] = resid[ROWS - 1]


def sum_all(values):
    return jnp.sum(jnp.sum(values, axis=0, keepdims=True), axis=1, keepdims=True)


def gram_row(fields, newest, base):
    lane = lanes((8, C))
    out = jnp.zeros((8, C), F32)
    for index, other in enumerate(fields):
        total = jnp.zeros((8, C), F32)
        for row in range(ROWS):
            total = total + jnp.sum((newest[row] * other[row]).reshape(N // 8, 8, C), axis=0)
        out = jnp.where(lane == base + index, sum_all(total), out)
    return out


def apply_kernel(count, shift, *refs):
    earlier, (slope, mix_hi, mix_lo, op_hi, op_lo, coeff, image, gram) = refs[:count], refs[count:]
    newest = earlier[-1]
    products = mix_products(mix_hi[...], mix_lo[...], [newest[row] for row in range(ROWS)])
    d = coeff[...]
    centre = 2.0 - shift[...]
    for row in range(ROWS):
        here = newest[row]
        image[row] = (
            products[row]
            + op_product(op_hi[row], op_lo[row], slope[row] * here)
            + (centre * here + d * local_lap(lambda r: newest[r], row))
        )
    gram[...] = gram_row(earlier, newest, count * (count - 1) // 2)


def finish_kernel(flags, image, coeff, up, down, left, right, vector, edges, first, last):
    halo = halo_terms(flags, up, down, left, right)
    d = coeff[...]
    for row in range(ROWS):
        vector[row] = image[row] - d * halo[row]
    edges[...] = edge_rows(lambda row: vector[row])
    first[...] = vector[0]
    last[...] = vector[ROWS - 1]


def last_kernel(flags, image, coeff, up, down, left, right, *refs):
    earlier, grams, (out, vector) = refs[:4], refs[4:8], refs[8:]
    halo = halo_terms(flags, up, down, left, right)
    d = coeff[...]
    for row in range(ROWS):
        vector[row] = image[row] - d * halo[row]
    total = gram_row(list(earlier) + [vector], vector, 10)
    for gram in grams:
        total = total + gram[...]
    out[...] = jnp.broadcast_to(total[:1], (128, C))


def combination(sums, shift):
    lane = lanes((1, C))
    width = ITERS + 1

    def entry(index):
        return jnp.sum(jnp.where(lane == index, sums, 0.0), axis=1, keepdims=True)

    gram = [[None] * width for _ in range(width)]
    for i in range(width):
        for j in range(i + 1):
            gram[i][j] = gram[j][i] = entry(i * (i + 1) // 2 + j)

    def times(vec):
        return [sum(gram[a][b] * vec[b] for b in range(width) if vec[b] is not None) for a in range(width)]

    def inner(vec, image):
        return sum(v * m for v, m in zip(vec, image) if v is not None)

    def less(vec, scale, other):
        return [v if o is None else (-scale * o if v is None else v - scale * o) for v, o in zip(vec, other)]

    beta = jnp.sqrt(gram[0][0] + 1e-12)
    basis = [[1.0 / beta] + [None] * ITERS]
    hess = {}
    worst = jnp.zeros((1, 1), F32)
    for step in range(ITERS):
        now = basis[-1]
        work = [None] * width
        for a in range(step + 2):
            moved = now[a - 1] if a > 0 else None
            kept = None if now[a] is None else shift * now[a]
            work[a] = moved if kept is None else (kept if moved is None else moved + kept)
        image = times(work)
        coefs = [inner(vec, image) for vec in basis]
        for index, coef in enumerate(coefs):
            hess[index, step] = coef
            work = less(work, coef, basis[index])
        square = inner(work, times(work))
        bound = sum(
            jnp.abs(work[a] * gram[a][b] * work[b]) for a in range(step + 2) for b in range(step + 2)
        )
        worst = jnp.where(bound <= AMP_MAX * square, worst, 1.0)
        length = jnp.sqrt(square + 1e-12)
        hess[step + 1, step] = length
        basis.append([None if v is None else v / length for v in work])

    normal = [[None] * ITERS for _ in range(ITERS)]
    for i in range(ITERS):
        for j in range(i + 1):
            normal[i][j] = sum(hess[k, i] * hess[k, j] for k in range(width) if (k, i) in hess and (k, j) in hess)
    factor = [[None] * ITERS for _ in range(ITERS)]
    for j in range(ITERS):
        value = normal[j][j]
        for k in range(j):
            value = value - factor[j][k] * factor[j][k]
        factor[j][j] = jnp.sqrt(value)
        for i in range(j + 1, ITERS):
            value = normal[i][j]
            for k in range(j):
                value = value - factor[i][k] * factor[j][k]
            factor[i][j] = value / factor[j][j]
    forward = []
    for i in range(ITERS):
        value = beta * hess[0, i]
        for k in range(i):
            value = value - factor[i][k] * forward[k]
        forward.append(value / factor[i][i])
    solved = [None] * ITERS
    for i in range(ITERS - 1, -1, -1):
        value = forward[i]
        for k in range(i + 1, ITERS):
            value = value - factor[k][i] * solved[k]
        solved[i] = value / factor[i][i]
    weights = []
    for a in range(ITERS):
        weights.append(sum(solved[i] * basis[i][a] for i in range(ITERS) if basis[i][a] is not None))
    total = sum(weights)
    worst = jnp.where(total - total == 0.0, worst, 1.0)
    return weights, worst


def update_kernel(shift, table, state, p0, p1, p2, p3, new_state, poor, held, sems):
    copies = [pltpu.make_async_copy(ref, held.at[i], sems.at[i]) for i, ref in enumerate((p0, p1, p2, p3, state))]
    for copy in copies:
        copy.start()
    sums = jnp.sum(table[...], axis=0, keepdims=True)
    weights, worst = combination(sums, shift[...])
    poor[...] = jnp.broadcast_to(worst, (1, C))
    for copy in copies:
        copy.wait()
    for row in range(ROWS):
        total = weights[0] * held[0, row]
        for index in range(1, ITERS):
            total = total + weights[index] * held[index, row]
        new_state[row] = held[ITERS, row] + total


def ring(size, step):
    return [(i, (i + step) % size) for i in range(size)]


def along(value, axis, step):
    return lax.ppermute(value, axis, ring(lax.axis_size(axis), step))


def partner(value):
    return along(value, "c", 1)


def exchange(edges, first, last):
    return along(last, GX, 1), along(first, GX, -1), along(edges, GY, 1), along(edges, GY, -1)


def spread_out(own):
    half = lax.rem(lax.axis_index("y") + lax.axis_index("z"), 2)
    mine = lax.dynamic_slice_in_dim(own, half * HALF, HALF, 0)
    low, high = along(mine, "x", 1), along(mine, "x", -1)
    top, bottom = along(low[: HALF // 2], "x", 1), along(high[HALF // 2 :], "x", -1)
    routes = (("y", 1), ("y", -1), ("z", 1), ("z", -1))
    sides = []
    for q, (axis, step) in enumerate(routes):
        rows = slice(q * PIECE, (q + 1) * PIECE)
        sides.append(along(jnp.stack([low[rows], high[rows]]), axis, step))
    ends = []
    for q, (axis, step) in enumerate(routes):
        source = (top, bottom)[q // 2]
        ends.append(along(source[(q % 2) * PIECE : (q % 2 + 1) * PIECE], axis, step))
    near = [own, low, high, top, bottom] + sides + ends
    return near, [partner(piece) for piece in near]


def total_sum(value):
    return lax.psum(value, ALL)


def careful(state, forcing, mix, diffusion, weights, own, regimes, flags):
    highest = lax.Precision.HIGHEST
    d = diffusion[None, :, None]
    gx, gy = lax.axis_size(GX), lax.axis_size(GY)
    keep = flags.astype(F32)
    here = lax.axis_index(GX)

    def passed(step, carry):
        moving, chosen = carry
        source = lax.rem(here - step + gx, gx)
        chosen = jnp.where((regimes == source)[:, None, None], moving[None], chosen)
        return lax.ppermute(moving, GX, ring(gx, 1)), chosen

    _, chosen = lax.fori_loop(0, gx, passed, (own, jnp.zeros((ROWS, N, N), F32)))

    def spread(field):
        up = lax.ppermute(field[-1:], GX, ring(gx, 1)) * keep[0]
        down = lax.ppermute(field[:1], GX, ring(gx, -1)) * keep[1]
        left = lax.ppermute(field[:, :, -1], GY, ring(gy, 1)) * keep[2]
        right = lax.ppermute(field[:, :, 0], GY, ring(gy, -1)) * keep[3]
        tall = jnp.concatenate([up, field, down], axis=0)
        wide = jnp.concatenate([left[:, :, None], field, right[:, :, None]], axis=2)
        lap = 4.0 * field - tall[2:] - tall[:-2] - wide[:, :, 2:] - wide[:, :, :-2]
        mixed = jnp.einsum("pq,xqy->xpy", mix, field, precision=highest)
        return 2.0 * field + mixed + d * lap

    def correct(field):
        return jnp.einsum("bpq,bqc->bpc", chosen, field, precision=highest) * weights

    shade = jnp.tanh(state)
    slope = 1.0 - shade * shade
    residual = forcing - (spread(state) + correct(shade))
    beta = jnp.sqrt(total_sum(jnp.sum(residual * residual)) + 1e-12)
    basis = jnp.zeros((ITERS + 1,) + FIELD, F32).at[0].set(residual / beta)

    def body(step, carry):
        basis, hess = carry
        current = lax.dynamic_index_in_dim(basis, step, 0, keepdims=False)
        image = spread(current) + correct(slope * current)
        coefs = total_sum(jnp.sum(basis * image[None], axis=(1, 2, 3)))
        image = image - jnp.sum(coefs[:, None, None, None] * basis, axis=0)
        length = jnp.sqrt(total_sum(jnp.sum(image * image)) + 1e-12)
        basis = lax.dynamic_update_index_in_dim(basis, image / length, step + 1, 0)
        column = jnp.where(jnp.arange(ITERS + 1) == step + 1, length, coefs)
        hess = jnp.where(jnp.arange(ITERS)[None, :] == step, column[:, None], hess)
        return basis, hess

    basis, hess = lax.fori_loop(0, ITERS, body, (basis, jnp.zeros((ITERS + 1, ITERS), F32)))
    gram = jnp.dot(hess.T, hess, precision=highest)
    target = beta * hess[0]
    factor = jnp.linalg.cholesky(gram)
    forward = []
    for i in range(ITERS):
        value = target[i]
        for k in range(i):
            value = value - factor[i, k] * forward[k]
        forward.append(value / factor[i, i])
    solved = [None] * ITERS
    for i in range(ITERS - 1, -1, -1):
        value = forward[i]
        for k in range(i + 1, ITERS):
            value = value - factor[k, i] * solved[k]
        solved[i] = value / factor[i, i]
    new_state = state
    for i in range(ITERS):
        new_state = new_state + solved[i] * basis[i]
    return new_state


def call(kernel, outs, ins, arrays, mib, flops, scratch=()):
    return pl.pallas_call(
        kernel,
        out_shape=outs,
        in_specs=ins,
        out_specs=[VM] * len(outs),
        scratch_shapes=list(scratch),
        compiler_params=params(mib),
        cost_estimate=cost(flops, 1 << 22),
    )(*arrays)


def local(state, forcing, vertical_mix, diffusion, column_class, block_regime, correction_ops):
    gx, gy = lax.axis_index(GX), lax.axis_index(GY)
    last_x, last_y = lax.axis_size(GX) - 1, lax.axis_size(GY) - 1
    flags = jnp.stack([gx > 0, gx < last_x, gy > 0, gy < last_y]).astype(jnp.int32)
    x, c, y, z = (lax.axis_index(axis) for axis in ALL)
    place = jnp.stack([x, c, lax.rem(y + z, 2)]).astype(jnp.int32)
    regimes = block_regime[0, :, 0]
    weights = (column_class.astype(F32) * 0.5)[:, None, :]
    coeff = diffusion[:, None]
    own = correction_ops[0]

    field = pltpu.VMEM(FIELD, F32)
    plane = pltpu.VMEM((N, C), F32)
    edge = pltpu.VMEM((8, N), F32)
    mm = 2 * N * N * ROWS * C

    near, far = spread_out(own)

    edges, first, last = call(edges_kernel, [edge, plane, plane], [VM], [state], 8, 1 << 20)
    edges, first, last, _ = lax.optimization_barrier((edges, first, last, near[1]))
    halo = exchange(edges, first, last)
    square = pltpu.VMEM((N, N), BF16)
    part, shade, slope, mix_hi, mix_lo, shift = call(
        prep_kernel,
        [field, field, field, square, square, pltpu.VMEM((1, 1), F32)],
        [VM] * 5,
        [state, forcing, vertical_mix, coeff, weights],
        20,
        3 * mm,
    )
    stack = pltpu.VMEM((ROWS, N, N), BF16)
    vector, edges, first, last, op_hi, op_lo = call(
        residual_kernel,
        [field, edge, plane, plane, stack, stack],
        [SM] * 3 + [VM] * 7 + [HB] * 26,
        [place, regimes, flags] + in_vmem(part, shade) + [coeff, *halo] + in_hbm(*near, *far),
        20,
        3 * mm,
        [pltpu.VMEM((ROWS, N, N), F32), pltpu.SemaphoreType.DMA((ROWS,))],
    )
    vectors, grams = [vector], []
    for step in range(ITERS):
        halo = exchange(edges, first, last)
        count = step + 1
        image, gram = call(
            functools.partial(apply_kernel, count),
            [field, pltpu.VMEM((8, C), F32)],
            [VM] * (count + 7),
            in_vmem(shift, *vectors, slope, mix_hi, mix_lo, op_hi, op_lo) + [coeff],
            16,
            6 * mm,
        )
        grams.append(gram)
        if step + 1 < ITERS:
            vector, edges, first, last = call(
                finish_kernel,
                [field, edge, plane, plane],
                [SM] + [VM] * 6,
                [flags] + in_vmem(image) + [coeff, *halo],
                8,
                1 << 20,
            )
            vectors.append(vector)
    sums = call(
        last_kernel,
        [jax.ShapeDtypeStruct((128, C), F32)],
        [SM] + [VM] * 14,
        [flags] + in_vmem(image) + [coeff, *halo] + in_vmem(*vectors, *grams),
        8,
        1 << 20,
        [pltpu.VMEM(FIELD, F32)],
    )[0]
    table = lax.all_to_all(sums, ALL, 0, 0, tiled=True)
    new_state, poor = call(
        update_kernel,
        [jax.ShapeDtypeStruct(FIELD, F32), jax.ShapeDtypeStruct((1, C), F32)],
        [VM] * 2 + [HB] * 5,
        [shift, table, state] + in_hbm(*vectors),
        20,
        1 << 20,
        [pltpu.VMEM((ITERS + 1,) + FIELD, F32), pltpu.SemaphoreType.DMA((ITERS + 1,))],
    )

    def again(_):
        return careful(state, forcing, vertical_mix, diffusion, weights, own, regimes, flags)

    return lax.cond(poor[0, 0] > 0.0, again, lambda kept: kept, new_state)


def solution(mesh):
    finer = Mesh(mesh.devices.reshape(4, 2, 4, 4), ALL)
    in_specs = (
        P(GX, None, GY),
        P(GX, None, GY),
        P(),
        P(),
        P(GX, GY),
        P(GY, GX, None),
        P(GX, None, None),
    )
    return jax.shard_map(local, mesh=finer, in_specs=in_specs, out_specs=P(GX, None, GY), check_vma=False)
```

```python
import functools

import jax
import jax.numpy as jnp
from jax import lax
from jax.experimental import pallas as pl
from jax.experimental.pallas import tpu as pltpu
from jax.sharding import Mesh
from jax.sharding import PartitionSpec as P

ITERS = 4
ROWS = 4
N = 768
C = 128
AMP_MAX = 1e4
ALL = ("x", "c", "y", "z")
GX = ("x", "c")
GY = ("y", "z")
HALF = N // 2
PIECE = N // 8
F32 = jnp.float32
BF16 = jnp.bfloat16
VM = pl.BlockSpec(memory_space=pltpu.VMEM)
SM = pl.BlockSpec(memory_space=pltpu.SMEM)
HB = pl.BlockSpec(memory_space=pltpu.HBM)
FIELD = (ROWS, N, C)


def params(mib):
    return pltpu.CompilerParams(vmem_limit_bytes=mib << 20)


def cost(flops, moved):
    return pl.CostEstimate(flops=flops, bytes_accessed=moved, transcendentals=0)


def in_vmem(*arrays):
    return [pltpu.with_memory_space_constraint(a, pltpu.VMEM) for a in arrays]


def in_hbm(*arrays):
    return [pltpu.with_memory_space_constraint(a, pltpu.HBM) for a in arrays]


def halves(value):
    high = value.astype(BF16)
    return high, (value - high.astype(F32)).astype(BF16)


def dot(left, right):
    return jnp.dot(left, right, preferred_element_type=F32)


def lanes(shape):
    return lax.broadcasted_iota(jnp.int32, shape, len(shape) - 1)


def folded(value):
    return value[:, :C] + value[:, C:]


def local_lap(field, row):
    here = field(row)
    lane = lanes((N, C))
    total = 4.0 * here
    if row > 0:
        total = total - field(row - 1)
    if row + 1 < ROWS:
        total = total - field(row + 1)
    left = jnp.where(lane == 0, 0.0, pltpu.roll(here, 1, 1))
    right = jnp.where(lane == C - 1, 0.0, pltpu.roll(here, C - 1, 1))
    return total - left - right


def halo_terms(flags, near_x, far_x, near_y, far_y):
    pick = lax.broadcasted_iota(jnp.int32, (8, N), 0) % 2 == 0
    odd_x, odd_y = flags[4] > 0, flags[5] > 0
    up = jnp.where(odd_x, near_x[...], far_x[...])
    down = jnp.where(odd_x, far_x[...], near_x[...])
    has_left = jnp.where(flags[2] > 0, jnp.where(odd_y, near_y[...], far_y[...]), 0.0)
    has_right = jnp.where(flags[3] > 0, jnp.where(odd_y, far_y[...], near_y[...]), 0.0)
    sides = jnp.concatenate([jnp.where(pick, has_left, has_right), jnp.zeros((C - 8, N), F32)], axis=0).T
    lane = lanes((N, C))
    out = []
    for row in range(ROWS):
        low = pltpu.roll(sides, (C - 2 * row) % C, 1)
        high = pltpu.roll(sides, (C - 1 - (2 * row + 1)) % C, 1)
        term = jnp.where(lane == 0, low, jnp.where(lane == C - 1, high, 0.0))
        if row == 0:
            term = term + jnp.where(flags[0] > 0, up, 0.0)
        if row == ROWS - 1:
            term = term + jnp.where(flags[1] > 0, down, 0.0)
        out.append(term)
    return out


def edge_rows(field):
    lane = lanes((N, C))
    tile = jnp.zeros((N, C), F32)
    for row in range(ROWS):
        moved = pltpu.roll(field(row), 2 * row + 1, 1)
        tile = jnp.where((lane == 2 * row) | (lane == 2 * row + 1), moved, tile)
    return tile.T[:8]


def mix_products(high, low, fields):
    splits = [halves(f) for f in fields]
    outs = [folded(dot(high, jnp.concatenate(s, axis=1))) for s in splits]
    for pair in range(0, ROWS, 2):
        both = dot(low, jnp.concatenate([splits[pair][0], splits[pair + 1][0]], axis=1))
        outs[pair] = outs[pair] + both[:, :C]
        outs[pair + 1] = outs[pair + 1] + both[:, C:]
    return outs


def op_product(high, low, field):
    fh, fl = halves(field)
    return folded(dot(high, jnp.concatenate([fh, fl], axis=1))) + dot(low, fh)


def to_neighbours(flags, vector, edges, near, far):
    edges[...] = edge_rows(lambda row: vector[row])
    near[...] = vector[(ROWS - 1) * (1 - flags[4])]
    far[...] = vector[(ROWS - 1) * flags[4]]


def edges_kernel(flags, state, edges, near, far):
    to_neighbours(flags, state, edges, near, far)


def prep_kernel(state, forcing, mix, coeff, weights, part, shade_out, slope_out, mix_hi, mix_lo, shift):
    whole = mix[...]
    high, low = halves(whole)
    mix_hi[...] = high
    mix_lo[...] = low
    diagonal = lax.broadcasted_iota(jnp.int32, (N, N), 0) == lanes((N, N))
    d = coeff[...]
    shift[...] = 2.0 + (4.0 * sum_all(d) + sum_all(jnp.where(diagonal, whole, 0.0))) / N
    products = mix_products(high, low, [state[row] for row in range(ROWS)])
    for row in range(ROWS):
        here = state[row]
        part[row] = forcing[row] - (2.0 * here + products[row] + d * local_lap(lambda r: state[r], row))
        shade = jnp.tanh(here)
        shade_out[row] = shade * weights[row]
        slope_out[row] = (1.0 - shade * shade) * weights[row]


def residual_kernel(place, regimes, flags, part, shade, coeff, near_x, far_x, near_y, far_y, *refs):
    near, far, rest = refs[:17], refs[17:34], refs[34:]
    resid, edges, near_row, far_row, op_hi, op_lo, held, sems = rest
    mine = pl.multiple_of(place[2] * HALF, HALF)
    other = pl.multiple_of(HALF - place[2] * HALF, HALF)

    def fetch(row, carry):
        regime = regimes[row]
        offset = lax.rem(lax.div(regime, 2) - place[0] + 4, 4)
        for same, pieces in ((True, near), (False, far)):
            here = (lax.rem(regime, 2) == place[1]) == same

            def take(source, start, rows):
                pltpu.make_async_copy(source, held.at[row, pl.ds(start, rows)], sems.at[row]).start()

            @pl.when(here & (offset == 0))
            def _():
                take(pieces[0], 0, N)

            for shift, at in ((3, 1), (1, 3)):

                @pl.when(here & (offset == shift))
                def _(at=at):
                    for index in range(2):
                        take(pieces[at + index], mine + index * HALF // 2, HALF // 2)
                        take(pieces[at + 8 + index], other + index * HALF // 2, HALF // 2)

            @pl.when(here & (offset == 2))
            def _():
                for index in range(4):
                    take(pieces[5 + index], mine + index * PIECE, PIECE)
                    take(pieces[13 + index], other + index * PIECE, PIECE)

        return carry

    lax.fori_loop(0, ROWS, fetch, 0)
    halo = halo_terms(flags, near_x, far_x, near_y, far_y)
    d = coeff[...]
    for row in range(ROWS):
        resid[row] = part[row] + d * halo[row]
    for row in range(ROWS):
        pltpu.make_async_copy(near[0], held.at[row], sems.at[row]).wait()
        high, low = halves(held[row])
        op_hi[row] = high
        op_lo[row] = low
        resid[row] = resid[row] - op_product(high, low, shade[row])
    to_neighbours(flags, resid, edges, near_row, far_row)


def sum_all(values):
    return jnp.sum(jnp.sum(values, axis=0, keepdims=True), axis=1, keepdims=True)


def gram_row(fields, newest, base):
    lane = lanes((8, C))
    out = jnp.zeros((8, C), F32)
    for index, other in enumerate(fields):
        total = jnp.zeros((8, C), F32)
        for row in range(ROWS):
            total = total + jnp.sum((newest[row] * other[row]).reshape(N // 8, 8, C), axis=0)
        out = jnp.where(lane == base + index, sum_all(total), out)
    return out


def apply_kernel(count, shift, *refs):
    earlier, (slope, mix_hi, mix_lo, op_hi, op_lo, coeff, image, gram) = refs[:count], refs[count:]
    newest = earlier[-1]
    products = mix_products(mix_hi[...], mix_lo[...], [newest[row] for row in range(ROWS)])
    d = coeff[...]
    centre = 2.0 - shift[...]
    for row in range(ROWS):
        here = newest[row]
        image[row] = (
            products[row]
            + op_product(op_hi[row], op_lo[row], slope[row] * here)
            + (centre * here + d * local_lap(lambda r: newest[r], row))
        )
    gram[...] = gram_row(earlier, newest, count * (count - 1) // 2)


def finish_kernel(flags, image, coeff, near_x, far_x, near_y, far_y, vector, edges, near, far):
    halo = halo_terms(flags, near_x, far_x, near_y, far_y)
    d = coeff[...]
    for row in range(ROWS):
        vector[row] = image[row] - d * halo[row]
    to_neighbours(flags, vector, edges, near, far)


def last_kernel(flags, image, coeff, near_x, far_x, near_y, far_y, *refs):
    earlier, grams, (out, vector) = refs[:4], refs[4:8], refs[8:]
    halo = halo_terms(flags, near_x, far_x, near_y, far_y)
    d = coeff[...]
    for row in range(ROWS):
        vector[row] = image[row] - d * halo[row]
    total = gram_row(list(earlier) + [vector], vector, 10)
    for gram in grams:
        total = total + gram[...]
    out[...] = jnp.broadcast_to(total[:1], (128, C))


def combination(sums, shift):
    lane = lanes((1, C))
    width = ITERS + 1

    def entry(index):
        return jnp.sum(jnp.where(lane == index, sums, 0.0), axis=1, keepdims=True)

    gram = [[None] * width for _ in range(width)]
    for i in range(width):
        for j in range(i + 1):
            gram[i][j] = gram[j][i] = entry(i * (i + 1) // 2 + j)

    def times(vec):
        return [sum(gram[a][b] * vec[b] for b in range(width) if vec[b] is not None) for a in range(width)]

    def inner(vec, image):
        return sum(v * m for v, m in zip(vec, image) if v is not None)

    def less(vec, scale, other):
        return [v if o is None else (-scale * o if v is None else v - scale * o) for v, o in zip(vec, other)]

    beta = jnp.sqrt(gram[0][0] + 1e-12)
    basis = [[1.0 / beta] + [None] * ITERS]
    hess = {}
    worst = jnp.zeros((1, 1), F32)
    for step in range(ITERS):
        now = basis[-1]
        work = [None] * width
        for a in range(step + 2):
            moved = now[a - 1] if a > 0 else None
            kept = None if now[a] is None else shift * now[a]
            work[a] = moved if kept is None else (kept if moved is None else moved + kept)
        image = times(work)
        coefs = [inner(vec, image) for vec in basis]
        for index, coef in enumerate(coefs):
            hess[index, step] = coef
            work = less(work, coef, basis[index])
        square = inner(work, times(work))
        bound = sum(
            jnp.abs(work[a] * gram[a][b] * work[b]) for a in range(step + 2) for b in range(step + 2)
        )
        worst = jnp.where(bound <= AMP_MAX * square, worst, 1.0)
        length = jnp.sqrt(square + 1e-12)
        hess[step + 1, step] = length
        basis.append([None if v is None else v / length for v in work])

    normal = [[None] * ITERS for _ in range(ITERS)]
    for i in range(ITERS):
        for j in range(i + 1):
            normal[i][j] = sum(hess[k, i] * hess[k, j] for k in range(width) if (k, i) in hess and (k, j) in hess)
    factor = [[None] * ITERS for _ in range(ITERS)]
    for j in range(ITERS):
        value = normal[j][j]
        for k in range(j):
            value = value - factor[j][k] * factor[j][k]
        factor[j][j] = jnp.sqrt(value)
        for i in range(j + 1, ITERS):
            value = normal[i][j]
            for k in range(j):
                value = value - factor[i][k] * factor[j][k]
            factor[i][j] = value / factor[j][j]
    forward = []
    for i in range(ITERS):
        value = beta * hess[0, i]
        for k in range(i):
            value = value - factor[i][k] * forward[k]
        forward.append(value / factor[i][i])
    solved = [None] * ITERS
    for i in range(ITERS - 1, -1, -1):
        value = forward[i]
        for k in range(i + 1, ITERS):
            value = value - factor[k][i] * solved[k]
        solved[i] = value / factor[i][i]
    weights = []
    for a in range(ITERS):
        weights.append(sum(solved[i] * basis[i][a] for i in range(ITERS) if basis[i][a] is not None))
    total = sum(weights)
    worst = jnp.where(total - total == 0.0, worst, 1.0)
    return weights, worst


def update_kernel(shift, table, state, p0, p1, p2, p3, new_state, poor, held, sems, sent):
    copies = [pltpu.make_async_copy(ref, held.at[i], sems.at[i]) for i, ref in enumerate((p0, p1, p2, p3, state))]
    for copy in copies:
        copy.start()
    sums = jnp.sum(table[...], axis=0, keepdims=True)
    weights, worst = combination(sums, shift[...])
    poor[...] = jnp.broadcast_to(worst, (1, C))
    for copy in copies:
        copy.wait()
    for row in range(ROWS):
        total = weights[0] * held[0, row]
        for index in range(1, ITERS):
            total = total + weights[index] * held[index, row]
        held[ITERS, row] = held[ITERS, row] + total
        pltpu.make_async_copy(held.at[ITERS, row], new_state.at[row], sent.at[row]).start()
    for row in range(ROWS):
        pltpu.make_async_copy(held.at[ITERS, row], new_state.at[row], sent.at[row]).wait()


def ring(size, step):
    return [(i, (i + step) % size) for i in range(size)]


def along(value, axis, step):
    return lax.ppermute(value, axis, ring(lax.axis_size(axis), step))


def partner(value):
    return along(value, "c", 1)


def swap(value, axis, first):
    size = lax.axis_size(axis)
    pairs = []
    for i in range(size):
        other = i + 1 if (i - first) % 2 == 0 else i - 1
        pairs.append((i, other if 0 <= other < size else i))
    return lax.ppermute(value, axis, pairs)


def exchange_x(near, far):
    return swap(near, GX, 0), swap(far, GX, 1)


def exchange_y(edges):
    return swap(edges, GY, 0), swap(edges, GY, 1)


def careful(state, forcing, mix, diffusion, weights, own, regimes, flags):
    highest = lax.Precision.HIGHEST
    d = diffusion[None, :, None]
    gx, gy = lax.axis_size(GX), lax.axis_size(GY)
    keep = flags.astype(F32)
    here = lax.axis_index(GX)

    def passed(step, carry):
        moving, chosen = carry
        source = lax.rem(here - step + gx, gx)
        chosen = jnp.where((regimes == source)[:, None, None], moving[None], chosen)
        return lax.ppermute(moving, GX, ring(gx, 1)), chosen

    _, chosen = lax.fori_loop(0, gx, passed, (own, jnp.zeros((ROWS, N, N), F32)))
    both = jnp.concatenate([jnp.broadcast_to(mix[None], chosen.shape), chosen], axis=2)

    def image_of(field, scaled):
        up = lax.ppermute(field[-1:], GX, ring(gx, 1)) * keep[0]
        down = lax.ppermute(field[:1], GX, ring(gx, -1)) * keep[1]
        left = lax.ppermute(field[:, :, -1], GY, ring(gy, 1)) * keep[2]
        right = lax.ppermute(field[:, :, 0], GY, ring(gy, -1)) * keep[3]
        tall = jnp.concatenate([up, field, down], axis=0)
        wide = jnp.concatenate([left[:, :, None], field, right[:, :, None]], axis=2)
        lap = 4.0 * field - tall[2:] - tall[:-2] - wide[:, :, 2:] - wide[:, :, :-2]
        stacked = jnp.concatenate([field, scaled * weights], axis=1)
        return 2.0 * field + jnp.einsum("bpq,bqc->bpc", both, stacked, precision=highest) + d * lap

    def body(step, carry):
        basis, table = carry
        current = lax.dynamic_index_in_dim(basis, jnp.maximum(step - 1, 0), 0, keepdims=False)
        shade = jnp.tanh(state)
        opening = step == 0
        field = jnp.where(opening, state, current)
        image = image_of(field, jnp.where(opening, shade, (1.0 - shade * shade) * current))
        image = jnp.where(opening, forcing - image, image)
        coefs = lax.psum(jnp.sum(basis * image[None], axis=(1, 2, 3)), ALL)
        image = image - jnp.sum(coefs[:, None, None, None] * basis, axis=0)
        length = jnp.sqrt(lax.psum(jnp.sum(image * image), ALL) + 1e-12)
        basis = lax.dynamic_update_index_in_dim(basis, image / length, step, 0)
        column = jnp.where(jnp.arange(ITERS + 1) == step, length, coefs)
        return basis, lax.dynamic_update_index_in_dim(table, column, step, 0)

    start = (jnp.zeros((ITERS + 1,) + FIELD, F32), jnp.zeros((ITERS + 1, ITERS + 1), F32))
    basis, table = lax.fori_loop(0, ITERS + 1, body, start)
    beta, hess = table[0, 0], table[1:].T
    gram = jnp.dot(hess.T, hess, precision=highest)
    target = beta * hess[0]
    factor = jnp.linalg.cholesky(gram)
    forward = []
    for i in range(ITERS):
        value = target[i]
        for k in range(i):
            value = value - factor[i, k] * forward[k]
        forward.append(value / factor[i, i])
    solved = [None] * ITERS
    for i in range(ITERS - 1, -1, -1):
        value = forward[i]
        for k in range(i + 1, ITERS):
            value = value - factor[k, i] * solved[k]
        solved[i] = value / factor[i, i]
    return state + jnp.sum(jnp.stack(solved)[:, None, None, None] * basis[:ITERS], axis=0)


def call(kernel, outs, ins, arrays, mib, flops, scratch=()):
    return pl.pallas_call(
        kernel,
        out_shape=outs,
        in_specs=ins,
        out_specs=[VM] * len(outs),
        scratch_shapes=list(scratch),
        compiler_params=params(mib),
        cost_estimate=cost(flops, 1 << 22),
    )(*arrays)


def local(state, forcing, vertical_mix, diffusion, column_class, block_regime, correction_ops):
    gx, gy = lax.axis_index(GX), lax.axis_index(GY)
    last_x, last_y = lax.axis_size(GX) - 1, lax.axis_size(GY) - 1
    x, c, y, z = (lax.axis_index(axis) for axis in ALL)
    flags = jnp.stack([gx > 0, gx < last_x, gy > 0, gy < last_y, c > 0, lax.rem(z, 2) > 0]).astype(jnp.int32)
    place = jnp.stack([x, c, lax.rem(y + z, 2)]).astype(jnp.int32)
    regimes = block_regime[0, :, 0]
    weights = (column_class.astype(F32) * 0.5)[:, None, :]
    coeff = diffusion[:, None]
    own = correction_ops[0]

    field = pltpu.VMEM(FIELD, F32)
    plane = pltpu.VMEM((N, C), F32)
    edge = pltpu.VMEM((8, N), F32)
    mm = 2 * N * N * ROWS * C

    half = lax.rem(y + z, 2)
    start = half * HALF
    upper = lax.dynamic_slice_in_dim(correction_ops, start, HALF // 2, 1)[0]
    lower = lax.dynamic_slice_in_dim(correction_ops, start + HALF // 2, HALF // 2, 1)[0]
    low_top, high_low = along(upper, "x", 1), along(lower, "x", -1)
    low_low, high_top = along(lower, "x", 1), along(upper, "x", -1)
    own_far = partner(own)
    edges, near, far = call(edges_kernel, [edge, plane, plane], [SM, VM], [flags, state], 8, 1 << 20)
    halo_y = exchange_y(edges)
    square = pltpu.VMEM((N, N), BF16)
    part, shade, slope, mix_hi, mix_lo, shift = call(
        prep_kernel,
        [field, field, field, square, square, pltpu.VMEM((1, 1), F32)],
        [VM] * 5,
        [state, forcing, vertical_mix, coeff, weights],
        20,
        3 * mm,
    )
    ends = [along(low_top[i * PIECE : (i + 1) * PIECE], "x", 1) for i in range(2)]
    ends += [along(high_low[i * PIECE : (i + 1) * PIECE], "x", -1) for i in range(2)]
    side_low_top, side_high_low = along(low_top, "y", 1), along(high_low, "z", 1)
    low_low, high_top, shift, *halo_y = lax.optimization_barrier((low_low, high_top, shift, *halo_y))
    side_low_low, side_high_top = along(low_low, "y", -1), along(high_top, "z", -1)
    near, far, _ = lax.optimization_barrier((near, far, low_low))
    halo_x = exchange_x(near, far)
    routes = (("y", 1), ("y", -1), ("z", 1), ("z", -1))
    turned = [along(end, *route) for end, route in zip(ends, routes)]
    turned[-1], *halo_x = lax.optimization_barrier((turned[-1], *halo_x))
    halo = (*halo_x, *halo_y)
    pieces = [low_top, low_low, high_top, high_low, *ends, side_low_top, side_low_low, side_high_top, side_high_low, *turned]
    pieces_far = [partner(piece) for piece in pieces]
    stack = pltpu.VMEM((ROWS, N, N), BF16)
    vector, edges, near, far, op_hi, op_lo = call(
        residual_kernel,
        [field, edge, plane, plane, stack, stack],
        [SM] * 3 + [VM] * 7 + [HB] * 34,
        [place, regimes, flags] + in_vmem(part, shade) + [coeff, *halo, own] + in_hbm(*pieces, own_far, *pieces_far),
        20,
        3 * mm,
        [pltpu.VMEM((ROWS, N, N), F32), pltpu.SemaphoreType.DMA((ROWS,))],
    )
    vectors, grams = [vector], []
    for step in range(ITERS):
        halo = exchange_x(near, far) + exchange_y(edges)
        count = step + 1
        image, gram = call(
            functools.partial(apply_kernel, count),
            [field, pltpu.VMEM((8, C), F32)],
            [VM] * (count + 7),
            in_vmem(shift, *vectors, slope, mix_hi, mix_lo, op_hi, op_lo) + [coeff],
            16,
            6 * mm,
        )
        grams.append(gram)
        if step + 1 < ITERS:
            vector, edges, near, far = call(
                finish_kernel,
                [field, edge, plane, plane],
                [SM] + [VM] * 6,
                [flags] + in_vmem(image) + [coeff, *halo],
                8,
                1 << 20,
            )
            vectors.append(vector)
    sums = call(
        last_kernel,
        [jax.ShapeDtypeStruct((128, C), F32)],
        [SM] + [VM] * 14,
        [flags] + in_vmem(image) + [coeff, *halo] + in_vmem(*vectors, *grams),
        8,
        1 << 20,
        [pltpu.VMEM(FIELD, F32)],
    )[0]
    table = lax.all_to_all(sums, ALL, 0, 0, tiled=True)
    new_state, poor = pl.pallas_call(
        update_kernel,
        out_shape=[pltpu.HBM(FIELD, F32), jax.ShapeDtypeStruct((1, C), F32)],
        in_specs=[VM] * 2 + [HB] * 5,
        out_specs=[HB, VM],
        scratch_shapes=[
            pltpu.VMEM((ITERS + 1,) + FIELD, F32),
            pltpu.SemaphoreType.DMA((ITERS + 1,)),
            pltpu.SemaphoreType.DMA((ROWS,)),
        ],
        compiler_params=params(20),
        cost_estimate=cost(1 << 20, 1 << 22),
    )(shift, table, state, *in_hbm(*vectors))

    def again(_):
        return careful(state, forcing, vertical_mix, diffusion, weights, own, regimes, flags)

    return lax.cond(poor[0, 0] > 0.0, again, lambda kept: kept, new_state)


def solution(mesh):
    finer = Mesh(mesh.devices.reshape(4, 2, 4, 4), ALL)
    in_specs = (
        P(GX, None, GY),
        P(GX, None, GY),
        P(),
        P(),
        P(GX, GY),
        P(GY, GX, None),
        P(GX, None, None),
    )
    return jax.shard_map(local, mesh=finer, in_specs=in_specs, out_specs=P(GX, None, GY), check_vma=False)
```
